32 devices in a mesh: rep: 4 (over x, core), tp: 8 (over z, y).
Axes of the slice: x: 2, y: 2, z: 4, core: 2. Of those that a mesh axis runs over, the one named last changes fastest.
Arguments:
- trainer_query: float32 [32, 256, 8192], P(('rep', 'tp')), may hold values from -6 to 6
- trainer_output: float32 [32, 8192, 256], P(('rep', 'tp')), may hold values from -6 to 6
- probes: bfloat16 [768, 8192], replicated, may hold values from -0.0625 to 0.0625
- shard_block: int32 [32], replicated, may hold values from 0 to 31, each once
- slice_owner: int32 [8], replicated, may hold values from 0 to 7, each once
Outputs:
- query_slices: bfloat16 [8, 8192, 1024], P('tp')
- output_slices: bfloat16 [8, 1024, 8192], P('tp')
- query_prints: float32 [8, 768, 1024], P('tp')
- output_prints: float32 [8, 1024, 768], P('tp')
The draws below stay inside these ranges and needn't reach their ends.
Inputs may be any that keep to these rules, and one draw needn't show every extreme that they name: `shard_block`: a permutation: each number once. `slice_owner`: a permutation: each number once.
All inputs are finite; a program needn't handle non-finite values.
Results may differ from the reference program's by a relative error of at most 0.0029.
Values may be sent and summed in bfloat16 or wider, within the bound.
A program may use at most 192 MiB of HBM per device.

```python
import jax
import jax.numpy as jnp

D = 8192
PROBES = 768
HQ = 8192
SHARD = 256
SLICE = 1024
N_TP = 8
DEVICES = 32


def shard_levels(rng, extent, shards, low, high):
    loudness = 1.0
    for dim, blocks in shards:
        heights = jax.random.uniform(jax.random.fold_in(jax.random.fold_in(rng, 6), dim), (blocks,), jnp.float32, low / len(shards), high / len(shards))
        loudness = loudness * jnp.repeat(jnp.exp(heights), extent[dim] // blocks).reshape((-1,) + (1,) * (len(extent) - 1 - dim))
    return loudness


def noise(stream_key, shape, deviation, reach, shards=(), kind=jnp.bfloat16):
    entries = deviation * jax.random.normal(stream_key, shape, jnp.float32)
    if shards:
        entries = entries * shard_levels(stream_key, shape, shards, -0.22, 0.18)
    return jnp.clip(entries, -reach, reach).astype(kind)


def setup_inputs(seed: int = 0) -> dict:
    streams_of = jax.random.split(jax.random.key(seed), 6)
    return {
        "trainer_query": noise(streams_of[0], (DEVICES, SHARD, HQ), 1.0, 6.0, ((0, 32),), jnp.float32),
        "trainer_output": noise(streams_of[1], (DEVICES, HQ, SHARD), 1.0, 6.0, ((0, 32),), jnp.float32),
        "probes": noise(streams_of[2], (PROBES, D), D ** -0.5, 0.0625),
        "shard_block": jax.random.permutation(streams_of[3], DEVICES).astype(jnp.int32),
        "slice_owner": jax.random.permutation(streams_of[4], N_TP).astype(jnp.int32),
    }


def reference(trainer_query, trainer_output, probes, shard_block, slice_owner):
    positions = jnp.arange(DEVICES, dtype=jnp.int32)
    inverse = jnp.zeros((DEVICES,), jnp.int32).at[shard_block].set(positions)
    query_full = trainer_query.astype(jnp.bfloat16)[inverse].reshape(D, HQ)
    output_full = jnp.transpose(trainer_output.astype(jnp.bfloat16)[inverse], (1, 0, 2)).reshape(HQ, D)
    query_slices = jnp.transpose(query_full.reshape(D, N_TP, SLICE)[:, slice_owner], (1, 0, 2))
    output_slices = output_full.reshape(N_TP, SLICE, D)[slice_owner]
    probe_wide = probes.astype(jnp.float32)
    query_prints = jnp.einsum("pd,jdc->jpc", probe_wide, query_slices.astype(jnp.float32))
    output_prints = jnp.einsum("jcd,pd->jcp", output_slices.astype(jnp.float32), probe_wide)
    return (query_slices, output_slices, query_prints, output_prints)
```

```python
import functools

import jax
import jax.numpy as jnp
from jax import lax
from jax.experimental import pallas as pl
from jax.experimental.pallas import tpu as pltpu
from jax.sharding import PartitionSpec as P

MESH = pl.DeviceIdType.MESH


def pack_kernel(owner_ref, query_ref, output_ref, query_blocks, output_blocks):
    query_blocks[...] = query_ref[...].astype(jnp.bfloat16)
    output_blocks[...] = output_ref[...].astype(jnp.bfloat16)


def pack(trainer_query, trainer_output, slice_owner):
    tp_count = slice_owner.shape[0]
    _, rows, width = trainer_query.shape
    cut = width // tp_count
    return pl.pallas_call(
        pack_kernel,
        out_shape=(
            jax.ShapeDtypeStruct((tp_count, rows, cut), jnp.bfloat16),
            jax.ShapeDtypeStruct((tp_count, cut, rows), jnp.bfloat16),
        ),
        grid_spec=pltpu.PrefetchScalarGridSpec(
            num_scalar_prefetch=1,
            grid=(tp_count,),
            in_specs=[
                pl.BlockSpec((1, rows, cut), lambda k, owner: (0, 0, owner[k])),
                pl.BlockSpec((1, cut, rows), lambda k, owner: (0, owner[k], 0)),
            ],
            out_specs=[
                pl.BlockSpec((1, rows, cut), lambda k, owner: (k, 0, 0)),
                pl.BlockSpec((1, cut, rows), lambda k, owner: (k, 0, 0)),
            ],
        ),
    )(slice_owner, trainer_query, trainer_output)


def pair_index(index, offset, count):
    paired, bit = 0, 1
    while bit < count:
        paired = paired + bit * lax.rem(lax.div(index, bit) + (offset // bit) % 2, 2)
        bit *= 2
    return paired


def move_kernel(
    rep_count, tp_count, lag, query_blocks, output_blocks, query_all, output_all,
    swap_send, swap_recv, near_send, near_recv, far_send, far_recv, own_sem,
):
    rep, tp = lax.axis_index("rep"), lax.axis_index("tp")
    partner = rep + 1 - 2 * lax.rem(rep, 2)
    hops = range(1, rep_count // 2)
    ahead = {hop: lax.rem(rep + 2 * hop, rep_count) for hop in hops}
    behind = {hop: lax.rem(rep + rep_count - 2 * hop, rep_count) for hop in hops}
    pairs = [pair_index(tp, offset, tp_count) for offset in range(tp_count)]
    arrays = ((query_blocks, query_all), (output_blocks, output_all))

    barrier = pltpu.get_barrier_semaphore()
    peers = [(rep, pairs[offset]) for offset in range(1, tp_count)]
    peers += [(partner, tp)] + [(ahead[hop], tp) for hop in hops]
    for peer in peers:
        pl.semaphore_signal(barrier, inc=1, device_id=peer, device_id_type=MESH)
    pl.semaphore_wait(barrier, len(peers))

    def send(source, target, send_sem, recv_sem, device):
        copy = pltpu.make_async_remote_copy(
            src_ref=source, dst_ref=target, send_sem=send_sem, recv_sem=recv_sem,
            device_id=device, device_id_type=MESH,
        )
        copy.start()
        return copy

    mine = rep * tp_count + tp
    swaps, nears, fars, owns = {}, {}, {}, []
    for offset in range(1, tp_count):
        for a, (blocks, everything) in enumerate(arrays):
            swaps[offset, a] = send(
                blocks.at[pairs[offset]], everything.at[mine],
                swap_send.at[a, offset], swap_recv.at[a, offset], (rep, pairs[offset]),
            )
    for a, (blocks, everything) in enumerate(arrays):
        own = pltpu.make_async_copy(blocks.at[tp], everything.at[mine], own_sem.at[a])
        own.start()
        owns.append(own)

    def spread(offset, a):
        blocks, everything = arrays[a]
        place = everything.at[rep * tp_count + pairs[offset]]
        if offset:
            swaps[offset, a].wait_recv()
            block = place
        else:
            block = blocks.at[tp]
        for hop in hops:
            fars[hop, offset, a] = send(
                block, place, far_send.at[hop - 1, a, offset], far_recv.at[hop - 1, a, offset],
                (ahead[hop], tp),
            )
        nears[0, offset, a] = send(
            block, place, near_send.at[0, a, offset], near_recv.at[0, a, offset], (partner, tp)
        )

    def relay(offset, a):
        for hop in hops:
            place = arrays[a][1].at[behind[hop] * tp_count + pairs[offset]]
            fars[hop, offset, a].wait_recv()
            nears[hop, offset, a] = send(
                place, place, near_send.at[hop, a, offset], near_recv.at[hop, a, offset],
                (partner, tp),
            )

    units = [(offset, a) for offset in range(tp_count) for a in range(2)]
    for step in range(len(units) + lag):
        if step < len(units):
            spread(*units[step])
        if step >= lag:
            relay(*units[step - lag])
    for copy in nears.values():
        copy.wait_recv()
    for copies in (swaps, fars, nears):
        for copy in copies.values():
            copy.wait_send()
    for own in owns:
        own.wait()


def move(query_blocks, output_blocks, rep_count):
    tp_count = query_blocks.shape[0]
    count = rep_count * tp_count
    half = rep_count // 2
    dma = pltpu.SemaphoreType.DMA
    return pl.pallas_call(
        functools.partial(move_kernel, rep_count, tp_count, 3),
        out_shape=(
            jax.ShapeDtypeStruct((count,) + query_blocks.shape[1:], jnp.bfloat16),
            jax.ShapeDtypeStruct((count,) + output_blocks.shape[1:], jnp.bfloat16),
        ),
        in_specs=[pl.BlockSpec(memory_space=pl.ANY)] * 2,
        out_specs=[pl.BlockSpec(memory_space=pl.ANY)] * 2,
        scratch_shapes=[
            dma((2, tp_count)), dma((2, tp_count)),
            dma((half, 2, tp_count)), dma((half, 2, tp_count)),
            dma((half - 1, 2, tp_count)), dma((half - 1, 2, tp_count)),
            dma((2,)),
        ],
        compiler_params=pltpu.CompilerParams(collective_id=0, has_side_effects=True),
    )(query_blocks, output_blocks)


def query_kernel(group, inverse_ref, *refs):
    blocks, (probes_ref, slice_ref, prints_ref) = refs[:group], refs[group:]
    rows = blocks[0].shape[1]
    for j, block in enumerate(blocks):
        slice_ref[0, j * rows : (j + 1) * rows, :] = block[0]
    part = jnp.dot(probes_ref[...], slice_ref[0], preferred_element_type=jnp.float32)

    @pl.when(pl.program_id(0) == 0)
    def _():
        prints_ref[0] = part

    @pl.when(pl.program_id(0) > 0)
    def _():
        prints_ref[0] += part


def output_kernel(group, inverse_ref, *refs):
    blocks, (probes_ref, slice_ref, prints_ref) = refs[:group], refs[group:]
    rows = blocks[0].shape[2]
    for j, block in enumerate(blocks):
        slice_ref[0, :, j * rows : (j + 1) * rows] = block[0]
    part = lax.dot_general(
        slice_ref[0], probes_ref[...], (((1,), (1,)), ((), ())),
        preferred_element_type=jnp.float32,
    )

    @pl.when(pl.program_id(0) == 0)
    def _():
        prints_ref[0] = part

    @pl.when(pl.program_id(0) > 0)
    def _():
        prints_ref[0] += part


def finish(body, everything, probes, inverse, slice_shape, prints_shape, along):
    count = everything.shape[0]
    block = everything.shape[1:]
    group = max(1, min(count, 1024 // block[along]))
    span = group * block[along]
    tile = list((1,) + block)
    tile[1 + along] = span
    in_specs = [
        pl.BlockSpec((1,) + block, lambda b, inv, j=j: (inv[b * group + j], 0, 0))
        for j in range(group)
    ]
    in_specs.append(pl.BlockSpec((probes.shape[0], span), lambda b, inv: (0, b)))
    place = (lambda b, inv: (0, b, 0)) if along == 0 else (lambda b, inv: (0, 0, b))
    return pl.pallas_call(
        functools.partial(body, group),
        out_shape=(
            jax.ShapeDtypeStruct(slice_shape, jnp.bfloat16),
            jax.ShapeDtypeStruct(prints_shape, jnp.float32),
        ),
        grid_spec=pltpu.PrefetchScalarGridSpec(
            num_scalar_prefetch=1,
            grid=(count // group,),
            in_specs=in_specs,
            out_specs=[
                pl.BlockSpec(tuple(tile), place),
                pl.BlockSpec(prints_shape, lambda b, inv: (0, 0, 0)),
            ],
        ),
    )(inverse, *([everything] * group), probes)


def per_device(trainer_query, trainer_output, probes, shard_block, slice_owner):
    tp_count = lax.axis_size("tp")
    rep_count = lax.axis_size("rep")
    count = tp_count * rep_count
    rows, width = trainer_query.shape[1:]
    cut = width // tp_count
    model = rows * count
    positions = jnp.arange(count, dtype=jnp.int32)
    held = shard_block[None, :] == positions[:, None]
    inverse = jnp.sum(jnp.where(held, positions[None, :], 0), axis=1, dtype=jnp.int32)
    query_blocks, output_blocks = pack(trainer_query, trainer_output, slice_owner)
    query_all, output_all = move(query_blocks, output_blocks, rep_count)
    query_slice, query_prints = finish(
        query_kernel, query_all, probes, inverse,
        (1, model, cut), (1, probes.shape[0], cut), 0,
    )
    output_slice, output_prints = finish(
        output_kernel, output_all, probes, inverse,
        (1, cut, model), (1, cut, probes.shape[0]), 1,
    )
    return query_slice, output_slice, query_prints, output_prints


def solution(mesh):
    placed = (P(("rep", "tp"), None, None), P(("rep", "tp"), None, None), P(), P(), P())
    return jax.shard_map(
        per_device,
        mesh=mesh,
        in_specs=placed,
        out_specs=(
            P("tp", None, None),
            P("tp", None, None),
            P("tp", None, None),
            P("tp", None, None),
        ),
        check_vma=False,
    )
```

```python
import functools

import jax
import jax.numpy as jnp
from jax import lax
from jax.experimental import pallas as pl
from jax.experimental.pallas import tpu as pltpu
from jax.sharding import PartitionSpec as P

MESH = pl.DeviceIdType.MESH


def pack_kernel(owner_ref, query_ref, output_ref, query_blocks, output_blocks):
    query_blocks[...] = query_ref[...].astype(jnp.bfloat16)
    output_blocks[...] = output_ref[...].astype(jnp.bfloat16)


def pack(trainer_query, trainer_output, slice_owner):
    tp_count = slice_owner.shape[0]
    _, rows, width = trainer_query.shape
    cut = width // tp_count
    return pl.pallas_call(
        pack_kernel,
        out_shape=(
            jax.ShapeDtypeStruct((tp_count, rows, cut), jnp.bfloat16),
            jax.ShapeDtypeStruct((tp_count, cut, rows), jnp.bfloat16),
        ),
        grid_spec=pltpu.PrefetchScalarGridSpec(
            num_scalar_prefetch=1,
            grid=(tp_count,),
            in_specs=[
                pl.BlockSpec((1, rows, cut), lambda k, owner: (0, 0, owner[k])),
                pl.BlockSpec((1, cut, rows), lambda k, owner: (0, owner[k], 0)),
            ],
            out_specs=[
                pl.BlockSpec((1, rows, cut), lambda k, owner: (k, 0, 0)),
                pl.BlockSpec((1, cut, rows), lambda k, owner: (k, 0, 0)),
            ],
        ),
    )(slice_owner, trainer_query, trainer_output)


def pair_index(index, offset, count):
    paired, bit = 0, 1
    while bit < count:
        low = lax.rem(lax.div(index, bit) + lax.div(offset, bit), 2)
        paired = paired + bit * low
        bit *= 2
    return paired


def move_kernel(rep_count, tp_count, multiply, *refs):
    if multiply:
        (owner_ref, query_blocks, output_blocks, probes_ref,
         query_all, output_all, query_prints, output_prints,
         swap_send, swap_recv, near_send, near_recv, far_send, far_recv, own_sem,
         probes, picked, query_tile, output_tile, load_sem, probes_sem) = refs
    else:
        (query_blocks, output_blocks, query_all, output_all,
         swap_send, swap_recv, near_send, near_recv, far_send, far_recv, own_sem) = refs
    rep, tp = lax.axis_index("rep"), lax.axis_index("tp")
    partner = rep + 1 - 2 * lax.rem(rep, 2)
    hops = range(1, rep_count // 2)
    ahead = {hop: lax.rem(rep + 2 * hop, rep_count) for hop in hops}
    behind = {hop: lax.rem(rep + rep_count - 2 * hop, rep_count) for hop in hops}
    across = {hop: lax.rem(partner + rep_count - 2 * hop, rep_count) for hop in hops}
    arrays = ((query_blocks, query_all), (output_blocks, output_all))
    mine = rep * tp_count + tp
    count = rep_count * tp_count
    rows = query_blocks.shape[1]

    def load_probes(block):
        columns = pl.ds(pl.multiple_of(block * rows, rows), rows)
        return pltpu.make_async_copy(
            probes_ref.at[:, columns], probes.at[block], probes_sem.at[block]
        )

    def pair(offset):
        return pair_index(tp, jnp.int32(offset), tp_count)

    barrier = pltpu.get_barrier_semaphore()
    peers = [(rep, pair(offset)) for offset in range(1, tp_count)]
    peers += [(partner, tp)] + [(ahead[hop], tp) for hop in hops]
    for peer in peers:
        pl.semaphore_signal(barrier, inc=1, device_id=peer, device_id_type=MESH)
    pl.semaphore_wait(barrier, len(peers))

    def remote(source, target, send_sem, recv_sem, device):
        return pltpu.make_async_remote_copy(
            src_ref=source, dst_ref=target, send_sem=send_sem, recv_sem=recv_sem,
            device_id=device, device_id_type=MESH,
        )

    def swap(offset, a):
        blocks, everything = arrays[a]
        return remote(
            blocks.at[pair(offset)], everything.at[mine],
            swap_send.at[a, offset], swap_recv.at[a, offset], (rep, pair(offset)),
        )

    def far(hop, offset, a, block, place):
        return remote(
            block, place, far_send.at[hop - 1, a, offset], far_recv.at[hop - 1, a, offset],
            (ahead[hop], tp),
        )

    def near(hop, offset, a, block, place):
        return remote(
            block, place, near_send.at[hop, a, offset], near_recv.at[hop, a, offset],
            (partner, tp),
        )

    def place_of(group, offset, a):
        return arrays[a][1].at[group * tp_count + pair(offset)]

    def own(a):
        blocks, everything = arrays[a]
        return pltpu.make_async_copy(blocks.at[tp], everything.at[mine], own_sem.at[a])

    def spread(offset, a, block):
        place = place_of(rep, offset, a)
        for hop in hops:
            far(hop, offset, a, block, place).start()
        near(0, offset, a, block, place).start()

    def relay(offset, a):
        for hop in hops:
            place = place_of(behind[hop], offset, a)
            far(hop, offset, a, place, place).wait_recv()
            near(hop, offset, a, place, place).start()

    def collect(offset, a):
        for hop in (0, *hops):
            place = place_of(rep, offset, a)
            near(hop, offset, a, place, place).wait_recv()

        @pl.when(offset == 0)
        def _():
            own(a).wait()
            if multiply and a == 0:

                @pl.loop(0, count)
                def _(block):
                    load_probes(block).wait()


        if not multiply:
            return
        groups = [rep, partner]
        for hop in hops:
            groups += [behind[hop], across[hop]]
        tile, prints = ((query_tile, query_prints), (output_tile, output_prints))[a]
        loads = []
        for j, group in enumerate(groups):
            spot = (pl.ds(j * rows, rows), slice(None))
            load = pltpu.make_async_copy(
                place_of(group, offset, a), tile.at[spot if a == 0 else spot[::-1]],
                load_sem.at[a, j],
            )
            load.start()
            loads.append(load)
        for j, group in enumerate(groups):
            owner = owner_ref[group * tp_count + pair(offset)]
            picked[:, j * rows : (j + 1) * rows] = probes[owner]
        for load in loads:
            load.wait()
        if a == 0:
            prints[0] += jnp.dot(picked[...], tile[...], preferred_element_type=jnp.float32)
        else:
            prints[0] += lax.dot_general(
                tile[...], picked[...], (((1,), (1,)), ((), ())),
                preferred_element_type=jnp.float32,
            )

    for offset in range(1, tp_count):
        for a in range(2):
            swap(offset, a).start()
    for a in range(2):
        spread(jnp.int32(0), a, arrays[a][0].at[tp])
    for a in range(2):
        own(a).start()
    if multiply:

        @pl.loop(0, count)
        def _(block):
            load_probes(block).start()

        query_prints[...] = jnp.zeros_like(query_prints)
        output_prints[...] = jnp.zeros_like(output_prints)

    @pl.loop(1, tp_count + 2)
    def _(step):
        for a in range(2):

            @pl.when(step < tp_count)
            def _():
                swap(step, a).wait_recv()
                spread(step, a, place_of(rep, step, a))

            @pl.when(step <= tp_count)
            def _():
                relay(step - 1, a)

            if a == 0:

                @pl.when(step >= 2)
                def _():
                    collect(step - 2, 1)

            else:

                @pl.when(step <= tp_count)
                def _():
                    collect(step - 1, 0)

    @pl.loop(0, tp_count)
    def _(offset):
        for a in range(2):

            @pl.when(offset > 0)
            def _():
                swap(offset, a).wait_send()

            place = place_of(rep, offset, a)
            for hop in hops:
                far(hop, offset, a, place, place).wait_send()
            for hop in (0, *hops):
                near(hop, offset, a, place, place).wait_send()


def move(query_blocks, output_blocks, probes, shard_block, rep_count, multiply):
    tp_count, rows, cut = query_blocks.shape
    count = rep_count * tp_count
    half = rep_count // 2
    kinds = probes.shape[0]
    dma = pltpu.SemaphoreType.DMA
    anywhere = pl.BlockSpec(memory_space=pl.ANY)
    shapes = [
        jax.ShapeDtypeStruct((count, rows, cut), jnp.bfloat16),
        jax.ShapeDtypeStruct((count, cut, rows), jnp.bfloat16),
    ]
    scratch = [
        dma((2, tp_count)), dma((2, tp_count)),
        dma((half, 2, tp_count)), dma((half, 2, tp_count)),
        dma((half - 1, 2, tp_count)), dma((half - 1, 2, tp_count)),
        dma((2,)),
    ]
    operands, in_specs, out_specs = [query_blocks, output_blocks], [anywhere] * 2, [anywhere] * 2
    if multiply:
        operands = [shard_block] + operands + [probes]
        in_specs = [pl.BlockSpec(memory_space=pltpu.SMEM)] + [anywhere] * 3
        out_specs += [pl.BlockSpec(memory_space=pltpu.VMEM)] * 2
        shapes += [
            jax.ShapeDtypeStruct((1, kinds, cut), jnp.float32),
            jax.ShapeDtypeStruct((1, cut, kinds), jnp.float32),
        ]
        scratch += [
            pltpu.VMEM((count, kinds, rows), jnp.bfloat16),
            pltpu.VMEM((kinds, rep_count * rows), jnp.bfloat16),
            pltpu.VMEM((rep_count * rows, cut), jnp.bfloat16),
            pltpu.VMEM((cut, rep_count * rows), jnp.bfloat16),
            dma((2, rep_count)),
            dma((count,)),
        ]
    return pl.pallas_call(
        functools.partial(move_kernel, rep_count, tp_count, multiply),
        out_shape=shapes,
        in_specs=in_specs,
        out_specs=out_specs,
        scratch_shapes=scratch,
        compiler_params=pltpu.CompilerParams(collective_id=0, has_side_effects=True),
    )(*operands)


def order_kernel(group, inverse_ref, *refs):
    queries, outputs = refs[:group], refs[group : 2 * group]
    query_slice, output_slice = refs[2 * group :]
    rows = queries[0].shape[1]
    for j in range(group):
        query_slice[0, j * rows : (j + 1) * rows, :] = queries[j][0]
        output_slice[0, :, j * rows : (j + 1) * rows] = outputs[j][0]


def order(query_all, output_all, inverse):
    count, rows, cut = query_all.shape
    group = max(1, min(count, 1024 // rows))
    picks = range(group)
    return pl.pallas_call(
        functools.partial(order_kernel, group),
        out_shape=(
            jax.ShapeDtypeStruct((1, count * rows, cut), jnp.bfloat16),
            jax.ShapeDtypeStruct((1, cut, count * rows), jnp.bfloat16),
        ),
        grid_spec=pltpu.PrefetchScalarGridSpec(
            num_scalar_prefetch=1,
            grid=(count // group,),
            in_specs=[
                pl.BlockSpec((1, rows, cut), lambda b, inv, j=j: (inv[b * group + j], 0, 0))
                for j in picks
            ]
            + [
                pl.BlockSpec((1, cut, rows), lambda b, inv, j=j: (inv[b * group + j], 0, 0))
                for j in picks
            ],
            out_specs=[
                pl.BlockSpec((1, group * rows, cut), lambda b, inv: (0, b, 0)),
                pl.BlockSpec((1, cut, group * rows), lambda b, inv: (0, 0, b)),
            ],
        ),
    )(inverse, *([query_all] * group), *([output_all] * group))


def query_kernel(group, inverse_ref, *refs):
    blocks, (probes_ref, slice_ref, prints_ref) = refs[:group], refs[group:]
    rows = blocks[0].shape[1]
    for j, block in enumerate(blocks):
        slice_ref[0, j * rows : (j + 1) * rows, :] = block[0]
    part = jnp.dot(probes_ref[...], slice_ref[0], preferred_element_type=jnp.float32)

    @pl.when(pl.program_id(0) == 0)
    def _():
        prints_ref[0] = part

    @pl.when(pl.program_id(0) > 0)
    def _():
        prints_ref[0] += part


def output_kernel(group, inverse_ref, *refs):
    blocks, (probes_ref, slice_ref, prints_ref) = refs[:group], refs[group:]
    rows = blocks[0].shape[2]
    for j, block in enumerate(blocks):
        slice_ref[0, :, j * rows : (j + 1) * rows] = block[0]
    part = lax.dot_general(
        slice_ref[0], probes_ref[...], (((1,), (1,)), ((), ())),
        preferred_element_type=jnp.float32,
    )

    @pl.when(pl.program_id(0) == 0)
    def _():
        prints_ref[0] = part

    @pl.when(pl.program_id(0) > 0)
    def _():
        prints_ref[0] += part


def finish(body, everything, probes, inverse, slice_shape, prints_shape, along):
    count = everything.shape[0]
    block = everything.shape[1:]
    group = max(1, min(count, 1024 // block[along]))
    span = group * block[along]
    tile = list((1,) + block)
    tile[1 + along] = span
    in_specs = [
        pl.BlockSpec((1,) + block, lambda b, inv, j=j: (inv[b * group + j], 0, 0))
        for j in range(group)
    ]
    in_specs.append(pl.BlockSpec((probes.shape[0], span), lambda b, inv: (0, b)))
    place = (lambda b, inv: (0, b, 0)) if along == 0 else (lambda b, inv: (0, 0, b))
    return pl.pallas_call(
        functools.partial(body, group),
        out_shape=(
            jax.ShapeDtypeStruct(slice_shape, jnp.bfloat16),
            jax.ShapeDtypeStruct(prints_shape, jnp.float32),
        ),
        grid_spec=pltpu.PrefetchScalarGridSpec(
            num_scalar_prefetch=1,
            grid=(count // group,),
            in_specs=in_specs,
            out_specs=[
                pl.BlockSpec(tuple(tile), place),
                pl.BlockSpec(prints_shape, lambda b, inv: (0, 0, 0)),
            ],
        ),
    )(inverse, *([everything] * group), probes)


def per_device(trainer_query, trainer_output, probes, shard_block, slice_owner):
    tp_count = lax.axis_size("tp")
    rep_count = lax.axis_size("rep")
    count = tp_count * rep_count
    rows, width = trainer_query.shape[1:]
    cut = width // tp_count
    model = rows * count
    positions = jnp.arange(count, dtype=jnp.int32)
    held = shard_block[None, :] == positions[:, None]
    inverse = jnp.sum(jnp.where(held, positions[None, :], 0), axis=1, dtype=jnp.int32)
    query_blocks, output_blocks = pack(trainer_query, trainer_output, slice_owner)
    multiply = rows % 128 == 0
    moved = move(query_blocks, output_blocks, probes, shard_block, rep_count, multiply)
    if multiply:
        query_all, output_all, query_prints, output_prints = moved
        query_slice, output_slice = order(query_all, output_all, inverse)
        return query_slice, output_slice, query_prints, output_prints
    query_all, output_all = moved
    query_slice, query_prints = finish(
        query_kernel, query_all, probes, inverse,
        (1, model, cut), (1, probes.shape[0], cut), 0,
    )
    output_slice, output_prints = finish(
        output_kernel, output_all, probes, inverse,
        (1, cut, model), (1, cut, probes.shape[0]), 1,
    )
    return query_slice, output_slice, query_prints, output_prints


def solution(mesh):
    placed = (P(("rep", "tp"), None, None), P(("rep", "tp"), None, None), P(), P(), P())
    return jax.shard_map(
        per_device,
        mesh=mesh,
        in_specs=placed,
        out_specs=(
            P("tp", None, None),
            P("tp", None, None),
            P("tp", None, None),
            P("tp", None, None),
        ),
        check_vma=False,
    )
```
